256 devices in a mesh: cell: 32 (over y_lo, z, core), tm: 8 (over y_hi, x).
Axes of the slice: x: 4, y: 4 (y_hi: 2, y_lo: 2; y = y_hi * 2 + y_lo), z: 8, core: 2. Of those that a mesh axis runs over, the one named last changes fastest.
Arguments:
- anomalies: float32 [65536, 8192], P('cell', 'tm'), may hold values from -6 to 6
- start_basis: float32 [8192, 128], P('tm'), may hold values from -0.0625 to 0.0625
Outputs:
- patterns: float32 [65536, 128], P(('cell', 'tm'))
The draws below stay inside these ranges and needn't reach their ends.
All inputs are finite; a program needn't handle non-finite values.
Results may differ from the reference program's by a relative error of at most 0.0003.
Values sent between devices are 32-bit elements; how exact they have to be, the bound alone decides.
No kernel may reach another device: no remote copies, remote signals or barrier semaphores. Data moves between devices by JAX's collectives and lax.ppermute only.
A program may use at most 64 MiB of HBM per device.

```python
import jax
import jax.numpy as jnp
from jax import lax

K = 128
ITERS = 2
CELLS = 65536
HOURS = 8192


def block_scale(stream_key, shape, split, low, high):
    def one(position, blocks):
        steps = jax.random.uniform(jax.random.fold_in(jax.random.fold_in(stream_key, 6), position), (blocks,), jnp.float32, low / len(split), high / len(split))
        return jnp.repeat(jnp.exp(steps), shape[position] // blocks).reshape((-1,) + (1,) * (len(shape) - position - 1))

    loudness = one(*split[0])
    for cut in split[1:]:
        loudness = loudness * one(*cut)
    return loudness


def gaussian(rng, extent, spread, limit, cuts=(), held_as=jnp.bfloat16):
    drawn = jax.random.normal(rng, extent, jnp.float32) * spread
    if len(cuts) > 0:
        drawn = block_scale(rng, extent, cuts, -0.22, 0.18) * drawn
    return jnp.clip(drawn, min=-limit, max=limit).astype(held_as)


def setup_inputs(seed: int = 0) -> dict:
    key_list = jax.random.split(jax.random.key(seed), 3)
    anomalies = gaussian(key_list[0], (CELLS, HOURS), 1.0, 6.0, ((0, 32), (1, 8)), jnp.float32)
    start_basis = gaussian(key_list[1], (HOURS, K), HOURS ** -0.5, 0.0625, ((0, 8),), jnp.float32)
    return dict(anomalies=anomalies, start_basis=start_basis)


def reference(anomalies, start_basis):
    full = lax.Precision.HIGHEST
    basis = start_basis
    for step in range(ITERS):
        spatial = jnp.dot(anomalies.astype(jnp.float32), basis.astype(jnp.float32), precision=full, preferred_element_type=jnp.float32)
        image = lax.dot_general(anomalies.astype(jnp.float32), spatial.astype(jnp.float32), (((0,), (0,)), ((), ())), precision=full, preferred_element_type=jnp.float32)
        gram = lax.dot_general(image.astype(jnp.float32), image.astype(jnp.float32), (((0,), (0,)), ((), ())), precision=full, preferred_element_type=jnp.float32)
        lower = jnp.linalg.cholesky(gram)
        basis = jax.scipy.linalg.solve_triangular(lower, image.T, lower=True).T
    return jnp.dot(anomalies.astype(jnp.float32), basis.astype(jnp.float32), precision=full, preferred_element_type=jnp.float32)
```

```python
import jax
import jax.numpy as jnp
from jax import lax
from jax.experimental import pallas as pl
from jax.experimental.pallas import tpu as pltpu
from jax.sharding import Mesh
from jax.sharding import PartitionSpec as P

K = 128
CELL = ("ylo", "z", "core")
RING = ("ylo", "z")
TM = ("yhi", "x")
F32 = jnp.float32
BF16 = jnp.bfloat16
FULL = lax.Precision.HIGHEST


def parts_of(value):
    high = value.astype(BF16)
    low = (value - high.astype(F32)).astype(BF16)
    return high, low


def dot(left, right):
    return jnp.dot(left, right, preferred_element_type=F32)


def full_dot(left, right, dims=((1,), (0,))):
    return lax.dot_general(left, right, (dims, ((), ())), precision=FULL, preferred_element_type=F32)


def times_basis(rows, wide):
    high, low = parts_of(rows)
    both = dot(high, wide) + dot(low, wide)
    return both[:, :K] + both[:, K:]


def first_product_kernel(a_ref, basis_ref, out_ref, wide_ref):
    @pl.when(pl.program_id(0) == 0)
    def _():
        wide_ref[:, :K], wide_ref[:, K:] = parts_of(basis_ref[...])

    out_ref[0] = times_basis(a_ref[...], wide_ref[...])


def first_product(a, basis, pieces):
    rows, hours = a.shape
    step = rows // pieces
    return pl.pallas_call(
        first_product_kernel,
        grid=(pieces,),
        in_specs=[
            pl.BlockSpec((step, hours), lambda i: (i, 0)),
            pl.BlockSpec((hours, K), lambda i: (0, 0)),
        ],
        out_specs=pl.BlockSpec((1, step, K), lambda i: (i, 0, 0)),
        out_shape=jax.ShapeDtypeStruct((pieces, step, K), F32),
        scratch_shapes=[pltpu.VMEM((hours, 2 * K), BF16)],
        cost_estimate=pl.CostEstimate(flops=8 * rows * hours * K, bytes_accessed=4 * rows * hours, transcendentals=0),
        name="first_product",
    )(a, basis)


def next_product_kernel(place_ref, a_ref, own_ref, other_ref, out_ref, wide_ref, gram_ref):
    core, seat = place_ref[0], place_ref[1]
    half = own_ref.shape[0]
    step = a_ref.shape[0]

    @pl.when(pl.program_id(0) == 0)
    def _():
        gram = jnp.zeros((K, K), F32)
        for ref, at in ((own_ref, core), (other_ref, 1 - core)):
            value = ref[...]
            high, low = parts_of(value)
            start = pl.multiple_of(at * half, half)
            wide_ref[pl.ds(start, half), :K] = high
            wide_ref[pl.ds(start, half), K:] = low
            gram = gram + full_dot(value, value, ((0,), (0,)))
        gram_ref[...] = gram

    out_ref[0, :step] = times_basis(a_ref[...], wide_ref[...])
    out_ref[0, step:] = gram_ref[pl.ds(pl.multiple_of(seat * 8, 8), 8), :]


def next_product(a, own, other, place, pieces):
    rows, hours = a.shape
    step = rows // pieces
    half = hours // 2
    return pl.pallas_call(
        next_product_kernel,
        grid_spec=pltpu.PrefetchScalarGridSpec(
            num_scalar_prefetch=1,
            grid=(pieces,),
            in_specs=[
                pl.BlockSpec((step, hours), lambda i, s: (i, 0)),
                pl.BlockSpec((half, K), lambda i, s: (0, 0)),
                pl.BlockSpec((half, K), lambda i, s: (0, 0)),
            ],
            out_specs=pl.BlockSpec((1, step + 8, K), lambda i, s: (i, 0, 0)),
            scratch_shapes=[pltpu.VMEM((hours, 2 * K), BF16), pltpu.VMEM((K, K), F32)],
        ),
        out_shape=jax.ShapeDtypeStruct((pieces, step + 8, K), F32),
        cost_estimate=pl.CostEstimate(flops=8 * rows * hours * K, bytes_accessed=4 * rows * hours, transcendentals=0),
        name="next_product",
    )(place, a, own, other)


def scaled_kernel(place_ref, own_ref, other_ref, scale_ref, basis_ref, gram_ref):
    core = place_ref[0]
    half = own_ref.shape[0]
    gram = jnp.zeros((K, K), F32)
    for ref, at in ((own_ref, core), (other_ref, 1 - core)):
        value = full_dot(ref[...], scale_ref[...])
        basis_ref[pl.ds(pl.multiple_of(at * half, half), half), :] = value
        gram = gram + full_dot(value, value, ((0,), (0,)))
    for i in range(gram_ref.shape[0]):
        gram_ref[i] = gram


def scaled(own, other, scale, place, copies):
    half = own.shape[0]
    vmem = pl.BlockSpec(memory_space=pltpu.VMEM)
    return pl.pallas_call(
        scaled_kernel,
        in_specs=[pl.BlockSpec(memory_space=pltpu.SMEM), vmem, vmem, vmem],
        out_specs=[vmem, vmem],
        out_shape=[
            jax.ShapeDtypeStruct((2 * half, K), F32),
            jax.ShapeDtypeStruct((copies, K, K), F32),
        ],
        name="scaled",
    )(place, own, other, scale)


def back_product_kernel(place_ref, a_ref, spatial_ref, send_ref, keep_ref, tall_ref):
    step = pl.program_id(0)

    @pl.when(step == 0)
    def _():
        width = spatial_ref.shape[2]
        for j in range(spatial_ref.shape[0]):
            high, low = parts_of(spatial_ref[j])
            tall_ref[:K, j * width : (j + 1) * width] = high
            tall_ref[K:, j * width : (j + 1) * width] = low

    high, low = parts_of(a_ref[...])
    tall = tall_ref[...]
    both = dot(tall, high) + dot(tall, low)
    value = (both[:K] + both[K:]).T

    @pl.when(step < 2)
    def _():
        send_ref[...] = value

    @pl.when(step >= 2)
    def _():
        keep_ref[...] = value


def back_product(a, spatial, place):
    rows, hours = a.shape
    width = hours // 4
    half = hours // 2
    return pl.pallas_call(
        back_product_kernel,
        grid_spec=pltpu.PrefetchScalarGridSpec(
            num_scalar_prefetch=1,
            grid=(4,),
            in_specs=[
                pl.BlockSpec((rows, width), lambda i, s: (0, (i + 2 * (1 - s[0])) % 4)),
                pl.BlockSpec(spatial.shape, lambda i, s: (0, 0, 0)),
            ],
            out_specs=[
                pl.BlockSpec((width, K), lambda i, s: (jnp.minimum(i, 1), 0)),
                pl.BlockSpec((width, K), lambda i, s: (jnp.maximum(i - 2, 0), 0)),
            ],
            scratch_shapes=[pltpu.VMEM((2 * K, rows), BF16)],
        ),
        out_shape=[jax.ShapeDtypeStruct((half, K), F32)] * 2,
        cost_estimate=pl.CostEstimate(flops=8 * rows * hours * K, bytes_accessed=4 * rows * hours, transcendentals=0),
        name="back_product",
    )(place, a, spatial)


def spread(line):
    return jnp.broadcast_to(line, (8, K))


def factor_kernel(gram_ref, out_ref, work_ref, pivot=4):
    rows = K // 8
    sub = lax.broadcasted_iota(jnp.int32, (8, K), 0)
    lane = lax.broadcasted_iota(jnp.int32, (8, K), 1)
    a = [gram_ref[8 * i : 8 * i + 8, :] for i in range(rows)]
    e = [(lane == sub + 8 * i).astype(F32) for i in range(rows)]
    diag = [jnp.zeros((8, K), F32) for _ in range(rows)]
    for first in range(0, K, pivot):
        b, top = divmod(first, 8)
        wide = {i: [spread(a[i][:, first + t : first + t + 1]) for t in range(pivot)] for i in range(b, rows)}
        line = [spread(a[b][top + t : top + t + 1, :]) for t in range(pivot)]
        unit = [spread(e[b][top + t : top + t + 1, :]) for t in range(pivot)]
        m = [[spread(wide[b][t][top + p : top + p + 1, :]) for t in range(pivot)] for p in range(pivot)]
        inverse = []
        for t in range(pivot):
            inverse.append(1.0 / m[t][t])
            for p in range(t + 1, pivot):
                ratio = m[p][t] * inverse[t]
                for q in range(t + 1, pivot):
                    m[p][q] = m[p][q] - ratio * m[t][q]
                line[p] = line[p] - ratio * line[t]
                unit[p] = unit[p] - ratio * unit[t]
        for i in range(b, rows):
            if i == b and top + pivot == 8:
                continue
            ratios = []
            for t in range(pivot):
                value = wide[i][t]
                for q in range(t):
                    value = value - ratios[q] * m[q][t]
                value = value * inverse[t]
                if i == b:
                    value = jnp.where(sub >= top + pivot, value, 0.0)
                ratios.append(value)
                a[i] = a[i] - value * line[t]
                e[i] = e[i] - value * unit[t]
        for t in range(pivot):
            e[b] = jnp.where(sub == top + t, unit[t], e[b])
            diag[b] = jnp.where(sub == top + t, m[t][t], diag[b])
    for i in range(rows):
        work_ref[8 * i : 8 * i + 8, :] = e[i] / jnp.sqrt(diag[i])
    out_ref[...] = work_ref[...].T


def inverse_factor(gram):
    return pl.pallas_call(
        factor_kernel,
        out_shape=jax.ShapeDtypeStruct((K, K), F32),
        scratch_shapes=[pltpu.VMEM((K, K), F32)],
        cost_estimate=pl.CostEstimate(flops=4_000_000, bytes_accessed=131072, transcendentals=0),
        name="factor",
    )(gram)


def traded(pieces, axes):
    return lax.all_to_all(pieces, axes, 0, 0, tiled=True)


def copied(value, axes):
    count = lax.axis_size(axes)
    return traded(jnp.broadcast_to(value[None], (count, *value.shape)), axes)


def swapped(value):
    return lax.ppermute(value, "core", [(0, 1), (1, 0)])


def on_device(anomalies, start_basis):
    place = jnp.stack([lax.axis_index("core"), lax.axis_index(RING)]).astype(jnp.int32)
    groups = lax.axis_size(TM)
    ring = lax.axis_size(RING)

    shared = traded(first_product(anomalies, start_basis, groups), TM).sum(axis=0)
    spatial = copied(shared.T, TM)
    send, keep = back_product(anomalies, spatial, place)
    arrived = traded((keep + swapped(send)).reshape(ring, -1, K), RING)
    own = copied(arrived.sum(axis=0), RING).reshape(-1, K)
    other = swapped(own)

    shared = traded(next_product(anomalies, own, other, place, groups), TM).sum(axis=0)
    spatial = copied(shared[:-8].T, TM)
    send, keep = back_product(anomalies, spatial, place)
    image = (keep + swapped(send)).reshape(ring, -1, K)
    lines = jnp.broadcast_to(shared[None, -8:], (ring, 8, K))
    arrived = traded(jnp.concatenate([image, lines], axis=1), RING)
    gram = arrived[:, -8:].reshape(K, K)
    own = copied(arrived[:, :-8].sum(axis=0), RING).reshape(-1, K)
    scale = inverse_factor(gram)
    other = swapped(own)
    image, gram = scaled(own, other, scale, place, groups)

    gram = traded(gram, TM).sum(axis=0)
    scale = inverse_factor(gram)
    shared = traded(first_product(anomalies, image, groups), TM).sum(axis=0)
    return full_dot(shared, scale)


def solution(mesh):
    fine = Mesh(mesh.devices.reshape(2, 8, 2, 2, 4), (*CELL, *TM))
    return jax.shard_map(
        on_device,
        mesh=fine,
        in_specs=(P(CELL, TM), P(TM, None)),
        out_specs=P((*CELL, *TM), None),
        check_vma=False,
    )
```
